32 devices in a mesh: dp: 4 (over y, x), tensor: 8 (over z, core).
Axes of the slice: x: 2, y: 2, z: 4, core: 2. Of those that a mesh axis runs over, the one named last changes fastest.
Arguments:
- tokens: bfloat16 [128, 4096], P(('dp', 'tensor')), may hold values from -6 to 6
- norm_gain: bfloat16 [4096], replicated, may hold values from 0.099609375 to 1.8984375
- gate_weight: bfloat16 [4096, 14336], P(None, 'tensor'), may hold values from -0.09375 to 0.09375
- up_weight: bfloat16 [4096, 14336], P(None, 'tensor'), may hold values from -0.09375 to 0.09375
- down_weight: bfloat16 [14336, 4096], P('tensor'), may hold values from -0.046875 to 0.046875
- drop_mask: int32 [128, 4096], P(('dp', 'tensor')), may hold values 0 or 1
- grad_bucket: bfloat16 [4, 2048, 512], P('dp', 'tensor'), may hold values from -6 to 6
Outputs:
- mixed: bfloat16 [128, 4096], P(('dp', 'tensor'))
- reduced: float32 [2048, 512], P('tensor', 'dp')
The draws below stay inside these ranges and needn't reach their ends.
All inputs are finite; a program needn't handle non-finite values. No bound on the sum of `drop_mask` on one device may be relied on, other than what follows from the above.
Results may differ from the reference program's by a relative error of at most 0.012.
Values may be sent and summed in bfloat16 or wider, within the bound.
A program may use at most 128 MiB of HBM per device.

```python
import jax
import jax.numpy as jnp
from jax import lax

D = 4096
FF = 14336
TOKENS = 128
GROWS = 2048
GCOLS = 512
N_DP = 4


def touch_ends(drawn, key, smallest, high):
    extent = drawn.shape
    index_at = [jax.random.randint(jax.random.fold_in(key, axis), (), 0, extent[axis]) for axis in range(len(extent))]
    drawn = drawn.at[tuple(index_at)].set(smallest)
    longest = extent.index(max(extent))
    index_at[longest] = (index_at[longest] + 1) % extent[longest]
    return drawn.at[tuple(index_at)].set(high)


def level_of(key, shape, cuts, low, top_value):
    def one(dim, blocks):
        steps = jax.random.uniform(jax.random.fold_in(jax.random.fold_in(key, 6), dim), (blocks,), jnp.float32, low / len(cuts), top_value / len(cuts))
        return jnp.repeat(jnp.exp(steps), shape[dim] // blocks).reshape((-1,) + (1,) * (len(shape) - dim - 1))

    loudness = one(*cuts[0])
    for cut in cuts[1:]:
        loudness = loudness * one(*cut)
    return loudness


def bell_draw(own_key, dims, width, most, pieces=(), held_as=jnp.bfloat16):
    gain = level_of(own_key, dims, pieces, -0.22, 0.18) if pieces else 1.0
    entries = jax.random.normal(own_key, dims, jnp.float32) * width * gain
    return jnp.minimum(jnp.maximum(entries, -most), most).astype(held_as)


def setup_inputs(seed: int = 0) -> dict:
    key_of = jax.random.split(jax.random.key(seed), 8)
    tokens = bell_draw(key_of[0], (TOKENS, D), 1.0, 6.0, ((0, 32),))
    norm_gain = jnp.clip(1.0 + 0.18 * jax.random.normal(key_of[1], (D,), jnp.float32), 0.099609375, 1.8984375).astype(jnp.bfloat16)
    gate_weight = bell_draw(key_of[2], (D, FF), D ** -0.5, 0.09375, ((1, 8),))
    up_weight = bell_draw(key_of[3], (D, FF), D ** -0.5, 0.09375, ((1, 8),))
    down_weight = bell_draw(key_of[4], (FF, D), FF ** -0.5, 0.046875, ((0, 8),))
    drop_mask = touch_ends((jax.random.randint(key_of[5], (TOKENS, D), 0, 10) < 9).astype(jnp.int32), jax.random.fold_in(key_of[5], 1), 0, 1)
    grad_bucket = bell_draw(key_of[6], (N_DP, GROWS, GCOLS), 1.0, 6.0, ((0, 4), (1, 8)))
    return dict(tokens=tokens, norm_gain=norm_gain, gate_weight=gate_weight, up_weight=up_weight, down_weight=down_weight, drop_mask=drop_mask, grad_bucket=grad_bucket)


def reference(tokens, norm_gain, gate_weight, up_weight, down_weight, drop_mask, grad_bucket):
    inputs = tokens.astype(jnp.float32)
    scale = lax.rsqrt(lax.optimization_barrier(jnp.mean(inputs * inputs, axis=-1, keepdims=True)) + 1e-05)
    normed = (inputs * scale * norm_gain.astype(jnp.float32)).astype(jnp.bfloat16)
    gate = jnp.dot(normed, gate_weight, preferred_element_type=jnp.float32)
    up_part = jnp.dot(normed, up_weight, preferred_element_type=jnp.float32)
    hidden = (jax.nn.silu(gate) * up_part).astype(jnp.bfloat16)
    branch = jnp.dot(hidden, down_weight, preferred_element_type=jnp.float32)
    mixed = (inputs + drop_mask.astype(jnp.float32) * branch / 0.9).astype(jnp.bfloat16)
    reduced = lax.optimization_barrier(jnp.sum(grad_bucket.astype(jnp.float32), axis=0))
    return (mixed, reduced)
```

```python
import functools

import jax
import jax.numpy as jnp
from jax import lax
from jax.experimental import pallas as pl
from jax.experimental.pallas import tpu as pltpu
from jax.sharding import PartitionSpec as P

MESH = pl.DeviceIdType.MESH
F32 = jnp.float32
BF16 = jnp.bfloat16
FIRST = 8


def split(size, most, unit):
    parts = most
    while parts > 1 and (size % parts or (size // parts) % unit):
        parts -= 1
    return parts


def kernel(
    n, m, kc, gc, dc, first,
    tok, gain, wg, wu, wd, mask, grad,
    mixed, reduced,
    vg, vu, vd, gath, gain_v, mask_v, acc_g, acc_u, hid, part, pair, comb, recv, gown, grecv,
):
    dma = pltpu.SemaphoreType.DMA
    half = n // 2
    pl.run_scoped(
        functools.partial(
            body, n, m, kc, gc, dc, first,
            tok, gain, wg, wu, wd, mask, grad, mixed, reduced,
            vg, vu, vd, gath, gain_v, mask_v, acc_g, acc_u, hid, part, pair, comb, recv, gown, grecv),
        dma((2 * kc + dc,)), dma((4,)), dma((gc, half)), dma((gc, n)), dma((gc, half)),
        dma((dc,)), dma((dc,)), dma((dc, half)), dma((dc, half)), dma((m,)), dma((m,)))


def body(
    n, m, kc, gc, dc, first,
    tok, gain, wg, wu, wd, mask, grad,
    mixed, reduced,
    vg, vu, vd, gath, gain_v, mask_v, acc_g, acc_u, hid, part, pair, comb, recv, gown, grecv,
    w_sem, l_sem, gs_sem, gr_sem, fs_sem, as_sem, ar_sem, ps_sem, pr_sem, bs_sem, br_sem,
):
    me = lax.axis_index("tensor")
    my_dp = lax.axis_index("dp")
    rows, width = tok.shape
    ffl = wg.shape[1]
    kd, gd, cd = width // kc, width // gc, width // dc
    gcols = reduced.shape[1]
    par = lax.rem(me, 2)
    chip = lax.div(me, 2)
    sib = me + 1 - 2 * par
    half = n // 2

    weights = []
    for k in range(kc):
        r = pl.ds(k * kd, kd)
        weights.append(pltpu.make_async_copy(wg.at[r], vg.at[r], w_sem.at[2 * k]))
        weights.append(pltpu.make_async_copy(wu.at[r], vu.at[r], w_sem.at[2 * k + 1]))
    for c in range(dc):
        r = pl.ds(c * cd, cd)
        weights.append(pltpu.make_async_copy(wd.at[:, r], vd.at[:, r], w_sem.at[2 * kc + c]))

    tok_copy = pltpu.make_async_copy(tok, gath.at[me], l_sem.at[0])
    tok_copy.start()
    gain_copy = pltpu.make_async_copy(gain, gain_v, l_sem.at[1])
    gain_copy.start()
    mask_copy = pltpu.make_async_copy(mask, mask_v, l_sem.at[2])
    mask_copy.start()
    own_copy = pltpu.make_async_copy(grad.at[0, :, pl.ds(pl.multiple_of(my_dp * gcols, 128), gcols)], gown, l_sem.at[3])
    own_copy.start()
    barrier = pltpu.get_barrier_semaphore()
    for k in range(1, n):
        pl.semaphore_signal(barrier, inc=1, device_id={"tensor": lax.rem(me + k, n)}, device_id_type=MESH)
    for k in range(1, m):
        pl.semaphore_signal(barrier, inc=1, device_id={"dp": lax.rem(my_dp + k, m)}, device_id_type=MESH)
    for w in weights[:first]:
        w.start()
    tok_copy.wait()
    pl.semaphore_wait(barrier, n + m - 2)

    def rows_to(g, slot, peer, send_sem):
        c = pl.ds(g * gd, gd)
        return pltpu.make_async_remote_copy(
            src_ref=gath.at[slot, :, c], dst_ref=gath.at[slot, :, c], send_sem=send_sem, recv_sem=gr_sem.at[g, slot],
            device_id={"tensor": peer}, device_id_type=MESH)

    sends = []
    for g in range(gc):
        for k in list(range(1, half)) + [0]:
            peer = lax.rem(me + 2 * k, n) if k else sib
            sends.append(rows_to(g, me, peer, gs_sem.at[g, k]))
            sends[-1].start()
    later = weights[first:]
    for w in later[:4]:
        w.start()
    buckets = []
    for k in range(1, m):
        peer = lax.rem(my_dp + k, m)
        buckets.append(pltpu.make_async_remote_copy(
            src_ref=grad.at[0, :, pl.ds(pl.multiple_of(peer * gcols, 128), gcols)], dst_ref=grecv.at[k - 1],
            send_sem=bs_sem.at[k - 1], recv_sem=br_sem.at[k - 1], device_id={"dp": peer}, device_id_type=MESH))
        buckets[-1].start()
    gain_copy.wait()

    def forward(g):
        for k in range(1, half):
            slot = lax.rem(me + n - 2 * k, n)
            rows_to(g, slot, me, gs_sem.at[g, k]).wait_recv()
            sends.append(rows_to(g, slot, sib, fs_sem.at[g, k]))
            sends[-1].start()

    q = 8 // rows
    squares = [jnp.zeros((8, 1), F32) for _ in range(n // q)]
    forward(0)
    for w in later[4:]:
        w.start()
    for g in range(gc):
        if g + 1 < gc:
            forward(g + 1)
        for k in range(half):
            rows_to(g, lax.rem(sib + n - 2 * k, n), me, fs_sem.at[g, 0]).wait_recv()
        gains = gain_v[pl.ds(g * gd, gd)].astype(F32).reshape(1, gd)
        blocks = []
        for p in range(n // q):
            v = jnp.concatenate([gath[q * p + i, :, pl.ds(g * gd, gd)].astype(F32) for i in range(q)], axis=0)
            squares[p] = squares[p] + jnp.sum(v * v, axis=-1, keepdims=True)
            blocks.append(v * gains)
        xg = jnp.concatenate(blocks, axis=0).astype(BF16)
        for k in range(g * kc // gc, (g + 1) * kc // gc):
            r = pl.ds(k * kd, kd)
            xk = xg[:, k * kd - g * gd:(k + 1) * kd - g * gd]
            for j, (v, acc) in enumerate(((vg, acc_g), (vu, acc_u))):
                weights[2 * k + j].wait()
                d = jnp.dot(xk, v[r, :], preferred_element_type=F32)
                acc[...] = d if k == 0 else acc[...] + d

    scale = lax.rsqrt(jnp.concatenate(squares, axis=0) / width + 1e-05)
    gate = acc_g[...] * scale
    hid[...] = (gate / (1.0 + jnp.exp(-gate)) * (acc_u[...] * scale)).astype(BF16)

    h = hid[...]
    pairs, parts = [], []

    def combine(c):
        r = pl.ds(c * cd, cd)
        pairs[c].wait_recv()
        for j in range(half):
            comb[j, :, r] = (part[par, j, :, r].astype(F32) + pair[j, :, r].astype(F32)).astype(BF16)
        for k in range(1, half):
            to = lax.rem(chip + k, half)
            parts.append(pltpu.make_async_remote_copy(
                src_ref=comb.at[to, :, r], dst_ref=recv.at[k - 1, :, r],
                send_sem=ps_sem.at[c, k], recv_sem=pr_sem.at[c, k],
                device_id={"tensor": 2 * to + par}, device_id_type=MESH))
            parts[-1].start()

    for c in range(dc):
        r = pl.ds(c * cd, cd)
        weights[2 * kc + c].wait()
        d = jnp.dot(h, vd[:, r], preferred_element_type=F32)
        for j in range(n):
            part[j % 2, j // 2, :, r] = d[rows * j:rows * (j + 1), :].astype(BF16)
        pairs.append(pltpu.make_async_remote_copy(
            src_ref=part.at[1 - par, :, :, r], dst_ref=pair.at[:, :, r],
            send_sem=as_sem.at[c], recv_sem=ar_sem.at[c],
            device_id={"tensor": sib}, device_id_type=MESH))
        pairs[-1].start()
        if c:
            combine(c - 1)
    combine(dc - 1)

    own_copy.wait()
    for b in buckets:
        b.wait_recv()
    total = gown[...].astype(F32)
    for k in range(m - 1):
        total = total + grecv[k].astype(F32)
    reduced[...] = total

    mask_copy.wait()
    for c in range(dc):
        r = pl.ds(c * cd, cd)
        total = comb[chip, :, r].astype(F32)
        for k in range(1, half):
            parts[c * (half - 1) + k - 1].wait_recv()
            total = total + recv[k - 1, :, r].astype(F32)
        mixed[:, r] = (gath[me, :, r].astype(F32) + mask_v[:, r].astype(F32) * total / 0.9).astype(BF16)
    for s in sends + buckets + pairs + parts:
        s.wait_send()


def store(mixed, reduced, mixed_out, reduced_out, sem):
    copies = [pltpu.make_async_copy(reduced, reduced_out, sem.at[0]), pltpu.make_async_copy(mixed, mixed_out, sem.at[1])]
    for c in copies:
        c.start()
    for c in copies:
        c.wait()


def per_device(n, m, tokens, norm_gain, gate_weight, up_weight, down_weight, drop_mask, grad_bucket):
    rows, width = tokens.shape
    ffl = gate_weight.shape[1]
    grows, gcols = grad_bucket.shape[1], grad_bucket.shape[2] // m
    kc, gc, dc = split(width, 4, 128), split(width, 4, 128), split(width, 4, 128)
    half = n // 2
    hbm = pl.BlockSpec(memory_space=pl.ANY)
    mixed, reduced = pl.pallas_call(
        functools.partial(kernel, n, m, kc, gc, dc, FIRST),
        name="ffn",
        out_shape=(pltpu.VMEM((rows, width), BF16), pltpu.VMEM((grows, gcols), F32)),
        in_specs=[hbm] * 7,
        out_specs=(pl.BlockSpec(memory_space=pltpu.VMEM),) * 2,
        scratch_shapes=[
            pltpu.VMEM((width, ffl), BF16),
            pltpu.VMEM((width, ffl), BF16),
            pltpu.VMEM((ffl, width), BF16),
            pltpu.VMEM((n, rows, width), BF16),
            pltpu.VMEM((width,), BF16),
            pltpu.VMEM((rows, width), jnp.int32),
            pltpu.VMEM((n * rows, ffl), F32),
            pltpu.VMEM((n * rows, ffl), F32),
            pltpu.VMEM((n * rows, ffl), BF16),
            pltpu.VMEM((2, half, rows, width), BF16),
            pltpu.VMEM((half, rows, width), BF16),
            pltpu.VMEM((half, rows, width), BF16),
            pltpu.VMEM((half - 1, rows, width), BF16),
            pltpu.VMEM((grows, gcols), BF16),
            pltpu.VMEM((m - 1, grows, gcols), BF16),
        ],
        compiler_params=pltpu.CompilerParams(
            collective_id=0, has_side_effects=True, vmem_limit_bytes=56 * 2**20),
    )(tokens, norm_gain, gate_weight, up_weight, down_weight, drop_mask, grad_bucket)
    return pl.pallas_call(
        store,
        name="store",
        out_shape=(jax.ShapeDtypeStruct((rows, width), BF16), jax.ShapeDtypeStruct((grows, gcols), F32)),
        in_specs=[pl.BlockSpec(memory_space=pltpu.VMEM)] * 2,
        out_specs=(hbm, hbm),
        scratch_shapes=[pltpu.SemaphoreType.DMA((2,))],
        compiler_params=pltpu.CompilerParams(vmem_limit_bytes=2**20),
    )(mixed, reduced)


def solution(mesh):
    return jax.shard_map(
        functools.partial(per_device, mesh.shape["tensor"], mesh.shape["dp"]),
        mesh=mesh,
        in_specs=(
            P(("dp", "tensor"), None),
            P(),
            P(None, "tensor"),
            P(None, "tensor"),
            P("tensor", None),
            P(("dp", "tensor"), None),
            P("dp", "tensor", None),
        ),
        out_specs=(P(("dp", "tensor"), None), P("tensor", "dp")),
        check_vma=False,
    )
```

```python
import functools

import jax
import jax.numpy as jnp
from jax import lax
from jax.experimental import pallas as pl
from jax.experimental.pallas import tpu as pltpu
from jax.sharding import PartitionSpec as P

MESH = pl.DeviceIdType.MESH
F32 = jnp.float32
BF16 = jnp.bfloat16
FIRST = 8
TILE = 256
EARLY = 99
LAG = 2
DIRECT = 1


def split(size, most, unit):
    parts = most
    while parts > 1 and (size % parts or (size // parts) % unit):
        parts -= 1
    return parts


def kernel(
    n, m, kc, gc, dc, first,
    tok, gain, wg, wu, wd, mask, grad,
    mixed, reduced,
    vg, vu, vd, gath, gain_v, mask_v, acc_g, acc_u, hid, part, pair, comb, recv, gown, grecv,
):
    dma = pltpu.SemaphoreType.DMA
    half = n // 2
    pl.run_scoped(
        functools.partial(
            body, n, m, kc, gc, dc, first,
            tok, gain, wg, wu, wd, mask, grad, mixed, reduced,
            vg, vu, vd, gath, gain_v, mask_v, acc_g, acc_u, hid, part, pair, comb, recv, gown, grecv),
        dma((2 * kc + dc,)), dma((4,)), dma((gc, half)), dma((gc, n)), dma((gc, half)),
        dma((dc,)), dma((dc,)), dma((dc, half)), dma((dc, half)), dma((m,)), dma((m,)))


def body(
    n, m, kc, gc, dc, first,
    tok, gain, wg, wu, wd, mask, grad,
    mixed, reduced,
    vg, vu, vd, gath, gain_v, mask_v, acc_g, acc_u, hid, part, pair, comb, recv, gown, grecv,
    w_sem, l_sem, gs_sem, gr_sem, fs_sem, as_sem, ar_sem, ps_sem, pr_sem, bs_sem, br_sem,
):
    me = lax.axis_index("tensor")
    my_dp = lax.axis_index("dp")
    rows, width = tok.shape
    ffl = wg.shape[1]
    kd, gd, cd = width // kc, width // gc, width // dc
    gcols = reduced.shape[1]
    par = lax.rem(me, 2)
    chip = lax.div(me, 2)
    sib = me + 1 - 2 * par
    half = n // 2

    weights = []
    for k in range(kc):
        r = pl.ds(k * kd, kd)
        weights.append(pltpu.make_async_copy(wg.at[r], vg.at[r], w_sem.at[2 * k]))
        weights.append(pltpu.make_async_copy(wu.at[r], vu.at[r], w_sem.at[2 * k + 1]))
    for c in range(dc):
        r = pl.ds(c * cd, cd)
        weights.append(pltpu.make_async_copy(wd.at[:, r], vd.at[:, r], w_sem.at[2 * kc + c]))

    tok_copy = pltpu.make_async_copy(tok, gath.at[me], l_sem.at[0])
    tok_copy.start()
    gain_copy = pltpu.make_async_copy(gain, gain_v, l_sem.at[1])
    gain_copy.start()
    mask_copy = pltpu.make_async_copy(mask, mask_v, l_sem.at[2])
    mask_copy.start()
    own_copy = pltpu.make_async_copy(grad.at[0, :, pl.ds(pl.multiple_of(my_dp * gcols, 128), gcols)], gown, l_sem.at[3])
    own_copy.start()
    barrier = pltpu.get_barrier_semaphore()
    for k in range(1, n):
        pl.semaphore_signal(barrier, inc=1, device_id={"tensor": lax.rem(me + k, n)}, device_id_type=MESH)
    for k in range(1, m):
        pl.semaphore_signal(barrier, inc=1, device_id={"dp": lax.rem(my_dp + k, m)}, device_id_type=MESH)
    for w in weights[:first]:
        w.start()
    tok_copy.wait()
    pl.semaphore_wait(barrier, n + m - 2)

    def rows_to(g, slot, peer, send_sem):
        c = pl.ds(g * gd, gd)
        return pltpu.make_async_remote_copy(
            src_ref=gath.at[slot, :, c], dst_ref=gath.at[slot, :, c], send_sem=send_sem, recv_sem=gr_sem.at[g, slot],
            device_id={"tensor": peer}, device_id_type=MESH)

    sends = []
    for g in range(gc):
        for k in list(range(1, half)) + [0]:
            peer = lax.rem(me + 2 * k, n) if k else sib
            sends.append(rows_to(g, me, peer, gs_sem.at[g, k]))
            sends[-1].start()
    later = weights[first:]
    for w in later[:4]:
        w.start()
    buckets = []
    for k in range(1, m):
        peer = lax.rem(my_dp + k, m)
        buckets.append(pltpu.make_async_remote_copy(
            src_ref=grad.at[0, :, pl.ds(pl.multiple_of(peer * gcols, 128), gcols)], dst_ref=grecv.at[k - 1],
            send_sem=bs_sem.at[k - 1], recv_sem=br_sem.at[k - 1], device_id={"dp": peer}, device_id_type=MESH))
        buckets[-1].start()
    gain_copy.wait()

    def forward(g):
        for k in range(1, half):
            slot = lax.rem(me + n - 2 * k, n)
            rows_to(g, slot, me, gs_sem.at[g, k]).wait_recv()
            sends.append(rows_to(g, slot, sib, fs_sem.at[g, k]))
            sends[-1].start()

    q = 8 // rows
    squares = [jnp.zeros((8, 1), F32) for _ in range(n // q)]
    forward(0)
    for w in later[4:]:
        w.start()
    for g in range(gc):
        if g + 1 < gc:
            forward(g + 1)
        for k in range(half):
            rows_to(g, lax.rem(sib + n - 2 * k, n), me, fs_sem.at[g, 0]).wait_recv()
        gains = gain_v[pl.ds(g * gd, gd)].astype(F32).reshape(1, gd)
        blocks = []
        for p in range(n // q):
            v = jnp.concatenate([gath[q * p + i, :, pl.ds(g * gd, gd)].astype(F32) for i in range(q)], axis=0)
            squares[p] = squares[p] + jnp.sum(v * v, axis=-1, keepdims=True)
            blocks.append(v * gains)
        xg = jnp.concatenate(blocks, axis=0).astype(BF16)
        for k in range(g * kc // gc, (g + 1) * kc // gc):
            r = pl.ds(k * kd, kd)
            xk = xg[:, k * kd - g * gd:(k + 1) * kd - g * gd]
            for j, (v, acc) in enumerate(((vg, acc_g), (vu, acc_u))):
                weights[2 * k + j].wait()
                d = jnp.dot(xk, v[r, :], preferred_element_type=F32)
                acc[...] = d if k == 0 else acc[...] + d

    scale = lax.rsqrt(jnp.concatenate(squares, axis=0) / width + 1e-05)
    gate = acc_g[...] * scale
    hid[...] = (gate / (1.0 + jnp.exp(-gate)) * (acc_u[...] * scale)).astype(BF16)

    h = hid[...]
    pairs, parts = [], []

    def combine(c):
        r = pl.ds(c * cd, cd)
        pairs[c].wait_recv()
        for j in range(half):
            comb[j, :, r] = (part[par, j, :, r].astype(F32) + pair[j, :, r].astype(F32)).astype(BF16)
        for k in range(1, half):
            to = lax.rem(chip + k, half)
            parts.append(pltpu.make_async_remote_copy(
                src_ref=comb.at[to, :, r], dst_ref=recv.at[k - 1, :, r],
                send_sem=ps_sem.at[c, k], recv_sem=pr_sem.at[c, k],
                device_id={"tensor": 2 * to + par}, device_id_type=MESH))
            parts[-1].start()

    for c in range(dc):
        r = pl.ds(c * cd, cd)
        weights[2 * kc + c].wait()
        d = jnp.dot(h, vd[:, r], preferred_element_type=F32)
        for j in range(n):
            part[j % 2, j // 2, :, r] = d[rows * j:rows * (j + 1), :].astype(BF16)
        pairs.append(pltpu.make_async_remote_copy(
            src_ref=part.at[1 - par, :, :, r], dst_ref=pair.at[:, :, r],
            send_sem=as_sem.at[c], recv_sem=ar_sem.at[c],
            device_id={"tensor": sib}, device_id_type=MESH))
        pairs[-1].start()
        if c:
            combine(c - 1)
    combine(dc - 1)

    own_copy.wait()
    for b in buckets:
        b.wait_recv()
    total = gown[...].astype(F32)
    for k in range(m - 1):
        total = total + grecv[k].astype(F32)
    reduced[...] = total

    mask_copy.wait()
    for c in range(dc):
        r = pl.ds(c * cd, cd)
        total = comb[chip, :, r].astype(F32)
        for k in range(1, half):
            parts[c * (half - 1) + k - 1].wait_recv()
            total = total + recv[k - 1, :, r].astype(F32)
        mixed[:, r] = (gath[me, :, r].astype(F32) + mask_v[:, r].astype(F32) * total / 0.9).astype(BF16)
    for s in sends + buckets + pairs + parts:
        s.wait_send()


def mxu_kernel(
    n, m, gc, dc,
    tok, gain, wg, wu, wd, mask, grad,
    mixed, reduced,
    vg, vu, vd, gath, gain_v, mask_v, xs, hid, part, pair, comb, recv, dpart, drecv, gown, grecv,
):
    dma = pltpu.SemaphoreType.DMA
    half, total_rows, tiles = n // 2, n * tok.shape[0], wg.shape[1] // TILE
    acc = [pltpu.ACC(q)((total_rows, TILE), F32) for _ in range(tiles) for q in (0, 1)]
    out = [pltpu.ACC(q)((total_rows, TILE), F32) for _ in range(wd.shape[1] // dc // TILE // 2) for q in (0, 1)]
    pl.run_scoped(
        functools.partial(
            mxu_body, n, m, gc, dc,
            tok, gain, wg, wu, wd, mask, grad, mixed, reduced,
            vg, vu, vd, gath, gain_v, mask_v, xs, hid, part, pair, comb, recv, dpart, drecv, gown, grecv),
        tuple(acc), tuple(out),
        dma((2 * gc + dc,)), dma((4,)), dma((gc, half)), dma((gc, n)), dma((gc, half)), dma((gc, half)),
        dma((dc,)), dma((dc,)), dma((dc, half)), dma((dc, half)), dma((n,)), dma((n,)), dma((m,)), dma((m,)))


def mxu_body(
    n, m, gc, dc,
    tok, gain, wg, wu, wd, mask, grad,
    mixed, reduced,
    vg, vu, vd, gath, gain_v, mask_v, xs, hid, part, pair, comb, recv, dpart, drecv, gown, grecv,
    acc, out,
    w_sem, l_sem, gs_sem, gr_sem, fs_sem, fr_sem, as_sem, ar_sem, ps_sem, pr_sem, ds_sem, dr_sem, bs_sem, br_sem,
):
    me = lax.axis_index("tensor")
    my_dp = lax.axis_index("dp")
    rows, width = tok.shape
    ffl = wg.shape[1]
    gd, cd = width // gc, width // dc
    gcols = reduced.shape[1]
    par = lax.rem(me, 2)
    chip = lax.div(me, 2)
    sib = me + 1 - 2 * par
    half = n // 2
    tiles, kb_g, kb_d = ffl // TILE, gd // TILE, ffl // TILE
    step = 2 * lax.div(chip, half // 2) - 1
    scope = jax.named_scope

    def far(i):
        return lax.rem(chip + step * i + half, half)

    tok_copy = pltpu.make_async_copy(tok, gath.at[me], l_sem.at[0])
    tok_copy.start()
    gain_copy = pltpu.make_async_copy(gain, gain_v, l_sem.at[1])
    gain_copy.start()
    mask_copy = pltpu.make_async_copy(mask, mask_v, l_sem.at[2])
    mask_copy.start()
    own_copy = pltpu.make_async_copy(grad.at[0, :, pl.ds(pl.multiple_of(my_dp * gcols, 128), gcols)], gown, l_sem.at[3])
    own_copy.start()
    barrier = pltpu.get_barrier_semaphore()
    for k in range(1, n):
        pl.semaphore_signal(barrier, inc=1, device_id={"tensor": lax.rem(me + k, n)}, device_id_type=MESH)
    for k in range(1, m):
        pl.semaphore_signal(barrier, inc=1, device_id={"dp": lax.rem(my_dp + k, m)}, device_id_type=MESH)
    weights = []
    for g in range(gc):
        r = pl.ds(g * gd, gd)
        weights.append(pltpu.make_async_copy(wg.at[r], vg.at[r], w_sem.at[2 * g]))
        weights.append(pltpu.make_async_copy(wu.at[r], vu.at[r], w_sem.at[2 * g + 1]))
    for c in range(dc):
        r = pl.ds(c * cd, cd)
        weights.append(pltpu.make_async_copy(wd.at[:, r], vd.at[:, r], w_sem.at[2 * gc + c]))
    for w in weights[:EARLY]:
        w.start()
    with scope("tok"):
        tok_copy.wait()
    with scope("barrier"):
        pl.semaphore_wait(barrier, n + m - 2)

    def rows_to(g, slot, peer, send_sem):
        c = pl.ds(g * gd, gd)
        return pltpu.make_async_remote_copy(
            src_ref=gath.at[slot, :, c], dst_ref=gath.at[slot, :, c], send_sem=send_sem, recv_sem=gr_sem.at[g, slot],
            device_id={"tensor": peer}, device_id_type=MESH)

    def chip_to(g, q):
        c, r = pl.ds(g * gd, gd), pl.ds(2 * q, 2)
        return pltpu.make_async_remote_copy(
            src_ref=gath.at[r, :, c], dst_ref=gath.at[r, :, c], send_sem=fs_sem.at[g, q], recv_sem=fr_sem.at[g, q],
            device_id={"tensor": sib}, device_id_type=MESH)

    sends = []
    for g in range(gc):
        for i in range(1, half):
            sends.append(rows_to(g, me, 2 * far(i) + 1, gs_sem.at[g, i]))
            sends[-1].start()
        sends.append(rows_to(g, me, sib, gs_sem.at[g, 0]))
        sends[-1].start()
    for w in weights[EARLY:]:
        w.start()
    buckets = []
    for k in range(1, m):
        peer = lax.rem(my_dp + k, m)
        buckets.append(pltpu.make_async_remote_copy(
            src_ref=grad.at[0, :, pl.ds(pl.multiple_of(peer * gcols, 128), gcols)], dst_ref=grecv.at[k - 1],
            send_sem=bs_sem.at[k - 1], recv_sem=br_sem.at[k - 1], device_id={"dp": peer}, device_id_type=MESH))
        buckets[-1].start()
    gain_copy.wait()

    def gather(g):
        with scope(f"gather{g}"):
            @pl.when(par == 1)
            def _():
                for i in range(half - 1, 0, -1):
                    q = far(i)
                    for p in range(2):
                        rows_to(g, 2 * q + p, me, gs_sem.at[g, i]).wait_recv()
                    chip_to(g, q).start()

            @pl.when(par == 0)
            def _():
                for i in range(half - 1, 0, -1):
                    chip_to(g, far(i)).wait_recv()
            rows_to(g, sib, me, gs_sem.at[g, 0]).wait_recv()

    per = 8 // rows
    groups = [[2 * (per * b + i) + p for i in range(per)] for p in range(2) for b in range(half // per)]
    squares = [jnp.zeros((8, 1), F32) for _ in groups]

    def norm(g):
        c = pl.ds(g * gd, gd)
        gains = gain_v[c].astype(F32).reshape(1, gd)
        blocks = []
        for b, slots in enumerate(groups):
            v = jnp.concatenate([gath[s, :, c].astype(F32) for s in slots], axis=0)
            squares[b] = squares[b] + jnp.sum(v * v, axis=-1, keepdims=True)
            blocks.append(v * gains)
        xs[:, c] = jnp.concatenate(blocks, axis=0).astype(BF16)

    turn = [0, 0]

    def multiply(q, to, left, right):
        pltpu.matmul_push_rhs(right, staging_register=turn[q], mxu_index=q)
        pltpu.matmul_acc_lhs(to, left, load_staged_rhs=turn[q])
        turn[q] = 1 - turn[q]

    def activate(t, scale):
        gate = pltpu.matmul_pop(acc[2 * t]) * scale
        up = pltpu.matmul_pop(acc[2 * t + 1]) * scale
        hid[:, pl.ds(t * TILE, TILE)] = (gate / (1.0 + jnp.exp(-gate)) * up).astype(BF16)

    gather(0)
    norm(0)
    scale = None
    for g in range(gc):
        with scope(f"w{g}"):
            weights[2 * g].wait()
            weights[2 * g + 1].wait()
        last = g == gc - 1
        if last:
            scale = lax.rsqrt(jnp.concatenate(squares, axis=0) / width + 1e-05)
        for t in range(tiles):
            f = pl.ds(t * TILE, TILE)
            for k in range(kb_g):
                r = pl.ds(g * gd + k * TILE, TILE)
                multiply(0, acc[2 * t], xs[:, r], vg[r, f])
                multiply(1, acc[2 * t + 1], xs[:, r], vu[r, f])
            if last and t:
                activate(t - 1, scale)
            if not last and t == tiles // 2:
                gather(g + 1)
                norm(g + 1)

    pairs, parts = [], []

    def combine(c):
        r = pl.ds(c * cd, cd)
        with scope(f"pair{c}"):
            pairs[c].wait_recv()
        both = part[par, :, r].astype(F32) + pair[:, r].astype(F32)
        for j in range(half):
            comb[j, :, r] = both[rows * j:rows * (j + 1), :].astype(BF16)
        for i in range(1, half):
            to = far(i)
            parts.append(pltpu.make_async_remote_copy(
                src_ref=comb.at[to, :, r], dst_ref=recv.at[chip, :, r],
                send_sem=ps_sem.at[c, i], recv_sem=pr_sem.at[c, chip],
                device_id={"tensor": 2 * to + par}, device_id_type=MESH))
            parts[-1].start()

    def part_of(c, q):
        r = pl.ds(c * cd, cd)
        return pltpu.make_async_remote_copy(
            src_ref=comb.at[q, :, r], dst_ref=recv.at[q, :, r],
            send_sem=ps_sem.at[c, 0], recv_sem=pr_sem.at[c, q],
            device_id={"tensor": sib}, device_id_type=MESH)

    def slot_to(slot, peer, i):
        return pltpu.make_async_remote_copy(
            src_ref=dpart.at[peer], dst_ref=drecv.at[slot],
            send_sem=ds_sem.at[i], recv_sem=dr_sem.at[slot],
            device_id={"tensor": peer}, device_id_type=MESH)

    half_rows = half * rows
    directs = []
    for c in range(dc):
        with scope(f"wd{c}"):
            weights[2 * gc + c].wait()
        pair_tiles = cd // TILE // 2
        for k in range(kb_d):
            if c == 0 and k == kb_d - 1:
                activate(tiles - 1, scale)
            r = pl.ds(k * TILE, TILE)
            for t in range(pair_tiles):
                for q in range(2):
                    multiply(q, out[2 * t + q], hid[:, r], vd[r, pl.ds(c * cd + (2 * t + q) * TILE, TILE)])
        for t in range(2 * pair_tiles):
            d = pltpu.matmul_pop(out[t])
            if c < dc - DIRECT:
                for p in range(2):
                    part[p, :, pl.ds(c * cd + t * TILE, TILE)] = d[p * half_rows:(p + 1) * half_rows, :].astype(BF16)
            else:
                for s in range(n):
                    at = (s % 2) * half_rows + (s // 2) * rows
                    dpart[s, :, pl.ds(t * TILE, TILE)] = d[at:at + rows, :].astype(BF16)
        if c < dc - DIRECT:
            r = pl.ds(c * cd, cd)
            pairs.append(pltpu.make_async_remote_copy(
                src_ref=part.at[1 - par, :, r], dst_ref=pair.at[:, r],
                send_sem=as_sem.at[c], recv_sem=ar_sem.at[c],
                device_id={"tensor": sib}, device_id_type=MESH))
            pairs[-1].start()
        else:
            for i in range(1, half):
                for p in range(2):
                    directs.append(slot_to(me, 2 * far(i) + p, 2 * i + p))
                    directs[-1].start()
            directs.append(slot_to(me, sib, 0))
            directs[-1].start()
        if c >= LAG and c - LAG < dc - DIRECT:
            combine(c - LAG)
        if c == dc // 2:
            with scope("bucket"):
                own_copy.wait()
                for b in buckets:
                    b.wait_recv()
            total = gown[...].astype(F32)
            for k in range(m - 1):
                total = total + grecv[k].astype(F32)
            reduced[...] = total
    for c in range(len(parts) // (half - 1), dc - DIRECT):
        combine(c)

    mask_copy.wait()

    def finish(c, total):
        r = pl.ds(c * cd, cd)
        mixed[:, r] = (gath[me, :, r].astype(F32) + mask_v[:, r].astype(F32) * total / 0.9).astype(BF16)

    for c in range(dc - DIRECT):
        r = pl.ds(c * cd, cd)
        total = comb[chip, :, r].astype(F32)
        with scope(f"part{c}"):
            for i in range(1, half):
                part_of(c, far(i)).wait_recv()
        for i in range(1, half):
            total = total + recv[far(i), :, r].astype(F32)
        finish(c, total)
    if DIRECT:
        total = dpart[me].astype(F32)
        with scope("direct"):
            slot_to(sib, me, 0).wait_recv()
            for i in range(half - 1, 0, -1):
                for p in range(2):
                    slot_to(2 * far(i) + p, me, 0).wait_recv()
        total = total + drecv[sib].astype(F32)
        for i in range(1, half):
            for p in range(2):
                total = total + drecv[2 * far(i) + p].astype(F32)
        finish(dc - 1, total)
    with scope("sent"):
        for s in sends + buckets + pairs + parts + directs:
            s.wait_send()

        @pl.when(par == 1)
        def _():
            for g in range(gc):
                for i in range(1, half):
                    chip_to(g, far(i)).wait_send()


def mxu_fits(n, rows, width, ffl):
    count = n * rows
    entries = count // 4 * (ffl // TILE + width // (8 * TILE))
    return (ffl % TILE == 0 and width % (16 * TILE) == 0 and count % 16 == 0 and 8 % rows == 0
            and n % 4 == 0 and (n // 2) * rows % 8 == 0 and entries <= 256)


def store(mixed, reduced, mixed_out, reduced_out, sem):
    copies = [pltpu.make_async_copy(reduced, reduced_out, sem.at[0]), pltpu.make_async_copy(mixed, mixed_out, sem.at[1])]
    for c in copies:
        c.start()
    for c in copies:
        c.wait()


def per_device(n, m, tokens, norm_gain, gate_weight, up_weight, down_weight, drop_mask, grad_bucket):
    rows, width = tokens.shape
    ffl = gate_weight.shape[1]
    grows, gcols = grad_bucket.shape[1], grad_bucket.shape[2] // m
    kc, gc, dc = split(width, 4, 128), split(width, 4, 128), split(width, 4, 128)
    half = n // 2
    hbm = pl.BlockSpec(memory_space=pl.ANY)
    common = [
        pltpu.VMEM((width, ffl), BF16),
        pltpu.VMEM((width, ffl), BF16),
        pltpu.VMEM((ffl, width), BF16),
        pltpu.VMEM((n, rows, width), BF16),
        pltpu.VMEM((width,), BF16),
        pltpu.VMEM((rows, width), jnp.int32),
    ]
    bucket = [pltpu.VMEM((grows, gcols), BF16), pltpu.VMEM((m - 1, grows, gcols), BF16)]
    if mxu_fits(n, rows, width, ffl):
        dc = split(width, 8, 2 * TILE)
        body = functools.partial(mxu_kernel, n, m, gc, dc)
        scratch = common + [
            pltpu.VMEM((n * rows, width), BF16),
            pltpu.VMEM((n * rows, ffl), BF16),
            pltpu.VMEM((2, half * rows, width), BF16),
            pltpu.VMEM((half * rows, width), BF16),
            pltpu.VMEM((half, rows, width), BF16),
            pltpu.VMEM((half, rows, width), BF16),
            pltpu.VMEM((n, rows, width // dc), BF16),
            pltpu.VMEM((n, rows, width // dc), BF16),
        ] + bucket
    else:
        body = functools.partial(kernel, n, m, kc, gc, dc, FIRST)
        scratch = common + [
            pltpu.VMEM((n * rows, ffl), F32),
            pltpu.VMEM((n * rows, ffl), F32),
            pltpu.VMEM((n * rows, ffl), BF16),
            pltpu.VMEM((2, half, rows, width), BF16),
            pltpu.VMEM((half, rows, width), BF16),
            pltpu.VMEM((half, rows, width), BF16),
            pltpu.VMEM((half - 1, rows, width), BF16),
        ] + bucket
    mixed, reduced = pl.pallas_call(
        body,
        name="ffn",
        out_shape=(pltpu.VMEM((rows, width), BF16), pltpu.VMEM((grows, gcols), F32)),
        in_specs=[hbm] * 7,
        out_specs=(pl.BlockSpec(memory_space=pltpu.VMEM),) * 2,
        scratch_shapes=scratch,
        compiler_params=pltpu.CompilerParams(
            collective_id=0, has_side_effects=True, vmem_limit_bytes=56 * 2**20),
    )(tokens, norm_gain, gate_weight, up_weight, down_weight, drop_mask, grad_bucket)
    return pl.pallas_call(
        store,
        name="store",
        out_shape=(jax.ShapeDtypeStruct((rows, width), BF16), jax.ShapeDtypeStruct((grows, gcols), F32)),
        in_specs=[pl.BlockSpec(memory_space=pltpu.VMEM)] * 2,
        out_specs=(hbm, hbm),
        scratch_shapes=[pltpu.SemaphoreType.DMA((2,))],
        compiler_params=pltpu.CompilerParams(vmem_limit_bytes=2**20),
    )(mixed, reduced)


def solution(mesh):
    return jax.shard_map(
        functools.partial(per_device, mesh.shape["tensor"], mesh.shape["dp"]),
        mesh=mesh,
        in_specs=(
            P(("dp", "tensor"), None),
            P(),
            P(None, "tensor"),
            P(None, "tensor"),
            P("tensor", None),
            P(("dp", "tensor"), None),
            P("dp", "tensor", None),
        ),
        out_specs=(P(("dp", "tensor"), None), P("tensor", "dp")),
        check_vma=False,
    )
```
